32 devices in a mesh: dom: 32 (over z, y, x, core).
Axes of the slice: x: 2, y: 2, z: 4, core: 2. Of those that a mesh axis runs over, the one named last changes fastest.
Arguments:
- right_side: float32 [1024, 16, 128], P('dom')
- band_blocks: float32 [1024, 5, 128, 128], P('dom'), as said below
- link_blocks: float32 [32, 6, 4, 128, 128], P('dom'), as said below
- link_rows: int32 [32, 6, 4], P('dom'), may hold values from 0 to 32, as said below
Outputs:
- solution: float32 [1024, 16, 128], P('dom')
- residual: float32 [1024, 16, 128], P('dom')
The draws below stay inside these ranges and needn't reach their ends.
Inputs may be any that keep to these rules, and one draw needn't show every extreme that they name: `link_rows`: entries are a row of device d (0 to 31) or 32 for an unused slot. Slot s of interface j of device d is paired with slot s of interface j xor 1 of the device it faces, and is used exactly when that one is. Each interface uses its first 1 to 4 slots and no row twice; in every draw some interface uses all 4. link_blocks[d, j, s] is the transpose of link_blocks[e, j xor 1, s] for the device e that interface j of d faces; blocks of unused slots are zero. band_blocks[g, 2 + m] is the transpose of band_blocks[g + m, 2 - m]; blocks whose column falls outside the device are zero. A is symmetric with a positive diagonal that exceeds the sum of magnitudes of the rest of its row.
All inputs are finite; a program needn't handle non-finite values.
Results may differ from the reference program's by a relative error of at most 0.0003.
Values sent between devices are 32-bit elements; how exact they have to be, the bound alone decides.
A program may use at most 64 MiB of HBM per device.

```python
import jax
import jax.numpy as jnp
from jax import lax

BS = 128
S = 16
R_DEV = 32
ITERS = 3
H = 4
NB = 1024
N_DOM = 32


def facing_offsets_drawn(dev_count):
    return (1, -1, dev_count // 16, -(dev_count // 16), dev_count // 4, -(dev_count // 4))


def rough_block(key, shape):
    weight = 1.0 / (7.0 * BS)
    spread = jax.random.uniform(key, shape, jnp.float32, 0.5, 1.5)
    return -weight * spread


def build_matrix(key):
    dev_count = N_DOM
    block_rows = R_DEV
    links = H
    offset_list = facing_offsets_drawn(dev_count)
    keys = jax.random.split(jax.random.fold_in(key, 11), 7)
    counts = jax.random.randint(keys[0], (dev_count, 3), 1, links + 1)
    fullest = jax.random.randint(keys[1], (3,), 0, dev_count)
    counts = counts.at[fullest, jnp.arange(3)].set(links)
    orders = jax.vmap(lambda sub: jax.random.permutation(sub, block_rows))(jax.random.split(keys[2], dev_count))
    slots = jnp.arange(links)
    used_list = []
    rows_list = []
    for facing in range(6):
        pair = facing // 2
        if facing % 2 == 0:
            owned = counts[:, pair]
        else:
            owned = jnp.roll(counts[:, pair], offset_list[facing - 1])
        used = slots[None, :] < owned[:, None]
        picked = orders[:, (facing * links + slots) % block_rows]
        used_list.append(used)
        rows_list.append(jnp.where(used, picked, block_rows).astype(jnp.int32))
    link_rows = jnp.stack(rows_list, axis=1)
    raw = rough_block(keys[3], (dev_count, 3, links, BS, BS))
    blocks_list = []
    for facing in range(6):
        pair = facing // 2
        kept = raw[:, pair] * used_list[2 * pair][:, :, None, None].astype(jnp.float32)
        if facing % 2 == 0:
            blocks_list.append(kept)
        else:
            blocks_list.append(jnp.roll(jnp.swapaxes(kept, -1, -2), offset_list[2 * pair], axis=0))
    link_blocks = jnp.stack(blocks_list, axis=1)
    upper = rough_block(keys[4], (dev_count, block_rows, 2, BS, BS))
    places = jnp.arange(block_rows)[:, None] + jnp.arange(1, 3)[None, :]
    upper = upper * (places < block_rows).astype(jnp.float32)[None, :, :, None, None]
    lower_one = jnp.swapaxes(jnp.roll(upper[:, :, 0], 1, axis=1), -1, -2)
    lower_two = jnp.swapaxes(jnp.roll(upper[:, :, 1], 2, axis=1), -1, -2)
    inner = rough_block(keys[5], (dev_count, block_rows, BS, BS))
    inner = 0.5 * (inner + jnp.swapaxes(inner, -1, -2))
    identity = jnp.eye(BS, dtype=jnp.float32)
    inner = inner * (1.0 - identity)
    row_abs = jnp.sum(jnp.abs(inner), axis=-1)
    row_abs = row_abs + jnp.sum(jnp.abs(upper), axis=(2, 4))
    row_abs = row_abs + jnp.sum(jnp.abs(lower_one), axis=-1) + jnp.sum(jnp.abs(lower_two), axis=-1)
    picks = (link_rows[:, :, :, None] == jnp.arange(block_rows)[None, None, None, :]).astype(jnp.float32)
    row_abs = row_abs + jnp.einsum('cjhr,cjhi->cri', picks, jnp.sum(jnp.abs(link_blocks), axis=-1))
    low, high = (0.05, 4.0)
    margin = jnp.exp(jax.random.uniform(keys[6], (dev_count, block_rows, BS), jnp.float32, jnp.log(low), jnp.log(high)))
    diagonal = inner + identity * (row_abs + margin)[..., :, None]
    band = jnp.stack([lower_two, lower_one, diagonal, upper[:, :, 0], upper[:, :, 1]], axis=2)
    return (link_rows, band.reshape(dev_count * block_rows, 5, BS, BS), link_blocks)


def draw_link_rows(key, part):
    return build_matrix(key)[0]


def draw_band_blocks(key, part):
    return build_matrix(key)[1]


def draw_link_blocks(key, part):
    return build_matrix(key)[2]


def draw_right_side(key, part):
    noise = jax.random.normal(jax.random.fold_in(key, 3), (NB, S, BS), jnp.float32)
    owner = (jnp.arange(NB) // R_DEV).astype(jnp.float32)
    rising = (1.0 + 2.0 * owner / (N_DOM - 1))[:, None, None]
    return noise * rising


def setup_inputs(seed: int = 0) -> dict:
    seeds = jax.random.split(jax.random.key(seed), 5)
    return {
        "right_side": draw_right_side(jax.random.fold_in(seeds[4], 71), 0),
        "band_blocks": draw_band_blocks(jax.random.fold_in(seeds[4], 71), 0),
        "link_blocks": draw_link_blocks(jax.random.fold_in(seeds[4], 71), 0),
        "link_rows": draw_link_rows(jax.random.fold_in(seeds[4], 71), 0),
    }


HIGHEST = lax.Precision.HIGHEST

def facing_offsets(dev_count):
    return (1, -1, dev_count // 16, -(dev_count // 16), dev_count // 4, -(dev_count // 4))

def apply_matrix(field, band_blocks, link_blocks, link_rows):
    dev_count = N_DOM
    block_rows = R_DEV
    shards = field.reshape(dev_count, block_rows, S, BS)
    padded = jnp.pad(shards, ((0, 0), (2, 2), (0, 0), (0, 0)))
    banded = band_blocks.reshape(dev_count, block_rows, 5, BS, BS)
    total = jnp.zeros_like(shards)
    for band_slot in range(5):
        total = total + jnp.einsum('nrsj,nrij->nrsi', padded[:, band_slot:band_slot + block_rows], banded[:, :, band_slot], precision=HIGHEST)
    extended = jnp.concatenate([shards, jnp.zeros((dev_count, 1, S, BS), field.dtype)], axis=1)
    devices = jnp.arange(dev_count, dtype=jnp.int32)
    offset_list = facing_offsets(dev_count)
    for facing in range(6):
        partner = ((devices + offset_list[facing]) % dev_count).astype(jnp.int32)
        far_rows = link_rows[partner, facing ^ 1]
        arrived = extended[partner[:, None], far_rows]
        contrib = jnp.einsum('nhsj,nhij->nhsi', arrived, link_blocks[:, facing], precision=HIGHEST)
        landing = jnp.zeros((dev_count, block_rows + 1, S, BS), field.dtype)
        landing = landing.at[devices[:, None], link_rows[:, facing]].add(contrib)
        total = total + landing[:, :block_rows]
    return total.reshape(NB, S, BS)

def gram_matrix(left, right):
    return jnp.einsum('nsi,nti->st', left, right, precision=HIGHEST)

def mix_columns(field, coeffs):
    return jnp.einsum('nsi,st->nti', field, coeffs, precision=HIGHEST)

def solve_gram(matrix, target):
    symmetric = 0.5 * (matrix + matrix.T)
    factor = jnp.linalg.cholesky(symmetric)
    return jax.scipy.linalg.cho_solve((factor, True), target)

def reference(right_side, band_blocks, link_blocks, link_rows):
    solution = jnp.zeros_like(right_side)
    residual = right_side
    direction = right_side
    squares = gram_matrix(residual, residual)
    for iteration in range(ITERS):
        image = apply_matrix(direction, band_blocks, link_blocks, link_rows)
        alpha = solve_gram(gram_matrix(direction, image), squares)
        solution = solution + mix_columns(direction, alpha)
        residual = residual - mix_columns(image, alpha)
        if iteration + 1 < ITERS:
            fresh = gram_matrix(residual, residual)
            beta = solve_gram(squares, fresh)
            direction = residual + mix_columns(direction, beta)
            squares = fresh
    return (solution, residual)
```

```python
import functools

import jax
import jax.numpy as jnp
from jax import lax
from jax.experimental import pallas as pl
from jax.experimental.pallas import tpu as pltpu
from jax.sharding import PartitionSpec as P

F32 = jnp.float32
BF16 = jnp.bfloat16
MESH = pl.DeviceIdType.MESH
CHUNK = 4
NFIELD = 10
R0, W0, Q0, R1, W1, Q1, D1, S1, R2, W2 = range(NFIELD)


def facing_offsets(dev_count):
    return (1, -1, dev_count // 16, -(dev_count // 16), dev_count // 4, -(dev_count // 4))


def split(x):
    hi = x.astype(BF16)
    lo = (x - hi.astype(F32)).astype(BF16)
    return hi, lo


def nn(a, b):
    return lax.dot_general(a, b, (((1,), (0,)), ((), ())), preferred_element_type=F32)


def nt(a, b):
    return lax.dot_general(a, b, (((1,), (1,)), ((), ())), preferred_element_type=F32)


def kernel(n, link_rows, rhs_hbm, band_hbm, link_hbm, sol, res,
           rhs, band, link, wt, lk, hl, wf, wband, hsend, hrecv0, hrecv1, hrecv2, gsend, gall, inv,
           load_sem, hs_sem, hr_sem, gs_sem, gr_sem):
    rows, s, bs = rhs.shape
    faces, slots = link.shape[:2]
    chunks = rows // CHUNK
    me = lax.axis_index("dom")
    offsets = facing_offsets(n)
    nslots = faces * slots
    hrecv = (hrecv0, hrecv1, hrecv2)

    rhs_copy = pltpu.make_async_copy(rhs_hbm, rhs, load_sem.at[0])
    link_copy = pltpu.make_async_copy(link_hbm.at[0], link, load_sem.at[1])

    def band_copy(c):
        at = pl.ds(c * CHUNK, CHUNK)
        return pltpu.make_async_copy(band_hbm.at[at], band.at[at], load_sem.at[2 + c])

    rhs_copy.start()
    link_copy.start()
    for c in range(chunks):
        band_copy(c).start()

    barrier = pltpu.get_barrier_semaphore()

    @pl.loop(1, n)
    def _(k):
        pl.semaphore_signal(barrier, inc=1, device_id=(lax.rem(me + k, n),), device_id_type=MESH)

    @pl.loop(0, rows)
    def _(r):
        for j in range(faces):
            found = jnp.int32(nslots)
            for t in range(slots):
                found = jnp.where(link_rows[0, j, t] == r, jnp.int32(j * slots + t), found)
            inv[r * faces + j] = found

    zero_pad = jnp.zeros((2 * s, bs), BF16)
    for f in (R0, W0, W1):
        for r in (0, 1, rows + 2, rows + 3):
            hl[f, r] = zero_pad
    zero_block = jnp.zeros((bs, 2 * bs), BF16)
    for r, m in ((2, 0), (2, 1), (3, 0), (rows, 4), (rows + 1, 3), (rows + 1, 4)):
        wt[r, m * bs:(m + 1) * bs, :] = zero_block
    for p in range(3):
        hrecv[p][nslots] = jnp.zeros((s, bs), F32)

    def put(f, r, x):
        hi, lo = split(x)
        hl[f, r + 2] = jnp.concatenate([hi, lo], axis=0)

    rhs_copy.wait()

    @pl.loop(0, rows // 4)
    def _(q):
        for u in range(4):
            r = q * 4 + u
            put(R0, r, rhs[r])

    link_copy.wait()

    @pl.loop(0, faces)
    def _(j):
        for t in range(slots):
            hi, lo = split(link[j, t])
            lk[j * slots + t] = jnp.concatenate([hi, lo], axis=1)

    def fold(x):
        half = x.shape[1] // 2
        y = x[:, :half] + x[:, half:]
        return y[:s] + y[s:]

    def halo(p, j):
        peer = lax.rem(me + offsets[j] + n, n)
        return pltpu.make_async_remote_copy(
            src_ref=hsend.at[p, pl.ds(j * slots, slots)],
            dst_ref=hrecv[p].at[pl.ds((j ^ 1) * slots, slots)],
            send_sem=hs_sem.at[p, j], recv_sem=hr_sem.at[p, j ^ 1],
            device_id=(peer,), device_id_type=MESH)

    def halo_arrived(p, j):
        return pltpu.make_async_remote_copy(
            src_ref=hsend.at[p, pl.ds(j * slots, slots)],
            dst_ref=hrecv[p].at[pl.ds(j * slots, slots)],
            send_sem=hs_sem.at[p, j], recv_sem=hr_sem.at[p, j],
            device_id=(me,), device_id_type=MESH)

    def halo_products(p, f):
        for j in range(faces):
            for t in range(slots):
                v = hl[f, link_rows[0, j, t] + 2]
                hsend[p, j * slots + t] = fold(nn(v, lk[j * slots + t]))

    def halo_start(p):
        for j in (4, 5, 2, 3, 0, 1):
            halo(p, j).start()

    def band_rows(f, first):
        for u in range(CHUNK):
            r = first + u
            v = jnp.concatenate([hl[f, r + m] for m in range(5)], axis=1)
            wband[r] = fold(nn(v, wt[r + 2]))

    def collect(p, f, keep):
        for j in range(faces):
            halo_arrived(p, j).wait_recv()

        @pl.loop(0, rows // 4)
        def _(q):
            for u in range(4):
                r = q * 4 + u
                w = wband[r]
                for j in range(faces):
                    w = w + hrecv[p][inv[r * faces + j]]
                if keep:
                    wf[r] = w
                put(f, r, w)

    lane = lax.broadcasted_iota(jnp.int32, (s, 128), 1)
    lane8 = lax.broadcasted_iota(jnp.int32, (s // 2, 128), 1)
    sub = lax.broadcasted_iota(jnp.int32, (s, 128), 0)

    def only(x):
        return jnp.where(lane < s, x, 0.0)

    def roll(x, by):
        return pltpu.roll(x, by % 128, 1)

    def gram_start(p, fr, fw, fd):
        def body(q, acc):
            for u in range(4):
                a, b = 4 * q + u + 2, 0
                right = jnp.concatenate(
                    [hl[fr, a], hl[fw, a], hl[fd, a], jnp.zeros((2 * s, bs), BF16)], axis=0)
                acc = acc + nt(right[:4 * s], right)
            return acc
        c = lax.fori_loop(0, rows // 4, body, jnp.zeros((4 * s, 128), F32))
        cr = c[:s] + c[s:2 * s]
        cw = c[2 * s:3 * s] + c[3 * s:]
        tr = cr + roll(cr, -s)
        tw = cw + roll(cw, -s)
        g = jnp.where(lane < s, tr, jnp.where(lane < 2 * s, roll(tw, -3 * s), jnp.where(lane < 3 * s, tr, 0.0)))
        msg = g[:s // 2] + roll(g[s // 2:], 64)
        gsend[p] = msg
        gall[p, me] = msg

        @pl.loop(1, n)
        def _(k):
            gram_copy(p, lax.rem(me + k, n), me, k).start()

    def gram_copy(p, peer, source, k):
        return pltpu.make_async_remote_copy(
            src_ref=gsend.at[p], dst_ref=gall.at[p, source],
            send_sem=gs_sem.at[p, k], recv_sem=gr_sem.at[p, source],
            device_id=(peer,), device_id_type=MESH)

    def gram_sum(p):
        @pl.loop(1, n)
        def _(k):
            source = lax.rem(me + k, n)
            gram_copy(p, source, source, k).wait_recv()
        total = jnp.sum(gall[p], axis=0)
        full = jnp.concatenate([jnp.where(lane8 < 64, total, 0.0),
                                jnp.where(lane8 < 64, roll(total, 64), 0.0)], axis=0)
        return only(full), only(roll(full, -s)), only(roll(full, -2 * s))

    def transpose(x):
        tall = jnp.concatenate([x, jnp.zeros((128 - s, 128), F32)], axis=0)
        return jnp.transpose(tall)[:s]

    def sym(x):
        return 0.5 * (x + transpose(x))

    def mul(a, b):
        return lax.dot_general(a[:, :s], b, (((1,), (0,)), ((), ())),
                               precision=lax.Precision.HIGHEST, preferred_element_type=F32)

    def solve(g, c):
        m = g + roll(c, s)
        for k in range(s):
            row = m[k:k + 1, :]
            scaled = row / row[:, k:k + 1]
            m = jnp.where(sub == k, scaled, m - m[:, k:k + 1] * scaled)
        return only(roll(m, -s))

    def mixer(blocks, outs):
        tall = [b for b in blocks for _ in range(2)]
        tall = tall + [jnp.zeros((128 - s * len(tall), 128), F32)]
        t = jnp.transpose(jnp.concatenate(tall, axis=0))[:outs * s, :2 * s * len(blocks)]
        hi, lo = split(t)
        return jnp.concatenate([hi, lo], axis=0)

    def mix(m, fields, r):
        u = jnp.concatenate([hl[f, r + 2] for f in fields], axis=0)
        y = nn(m, u)
        half = y.shape[0] // 2
        return y[:half] + y[half:]

    halo_products(0, R0)
    pl.semaphore_wait(barrier, n - 1)
    halo_start(0)

    def convert(c):
        band_copy(c).wait()

        @pl.loop(0, CHUNK)
        def _(u):
            h = c * CHUNK + u
            for b in range(5):
                hi, lo = split(band[h, b])
                wt[h + b, (4 - b) * bs:(5 - b) * bs, :bs] = hi
                wt[h + b, (4 - b) * bs:(5 - b) * bs, bs:] = lo

    convert(0)

    @pl.loop(1, chunks)
    def _(c):
        convert(c)
        band_rows(R0, (c - 1) * CHUNK)

    band_rows(R0, rows - CHUNK)
    collect(0, W0, True)
    gram_start(0, R0, W0, R0)

    def apply(p, fin, fout):
        halo_products(p, fin)
        halo_start(p)

        @pl.loop(0, rows // CHUNK)
        def _(q):
            band_rows(fin, q * CHUNK)
        collect(p, fout, False)

    apply(1, W0, Q0)
    rr, _, rw = gram_sum(0)
    rr0 = sym(rr)
    k0 = sym(rw)
    alpha = solve(k0, rr0)
    m0 = mixer([alpha], 1)

    @pl.loop(0, rows // 2)
    def _(q):
        for u in range(2):
            r = q * 2 + u
            sol[r] = mix(m0, [R0], r)
            x = rhs[r] - mix(m0, [W0], r)
            res[r] = x
            put(R1, r, x)
            w = wf[r] - mix(m0, [Q0], r)
            wf[r] = w
            put(W1, r, w)

    gram_start(1, R1, W1, R0)
    eye = jnp.where(sub == lane, 1.0, 0.0).astype(F32)
    inv0 = solve(rr0, eye)
    apply(2, W1, Q1)

    def coefficients(p, inverse, curv):
        rr, wd, rw = gram_sum(p)
        fresh = sym(rr)
        beta = mul(inverse, fresh)
        beta_t = mul(fresh, inverse)
        curv = sym(rw + mul(2.0 * wd + mul(beta_t, curv), beta))
        alpha = solve(curv, fresh)
        return fresh, curv, beta, alpha, mul(beta, alpha)

    rr1, k1, beta, alpha, gamma = coefficients(1, inv0, k0)
    m1 = mixer([beta + roll(gamma, s), roll(alpha, s)], 2)

    @pl.loop(0, rows // 2)
    def _(q):
        for u in range(2):
            r = q * 2 + u
            y = mix(m1, [R0, R1], r)
            put(D1, r, res[r] + y[:s])
            sol[r] = sol[r] + y[s:]
            y = mix(m1, [W0, W1], r)
            put(S1, r, wf[r] + y[:s])
            x = res[r] - y[s:]
            res[r] = x
            put(R2, r, x)
            y = mix(m1, [Q0, Q1], r)
            put(W2, r, wf[r] - y[s:])

    gram_start(2, R2, W2, D1)
    inv1 = solve(rr1, eye)
    _, _, _, alpha, gamma = coefficients(2, inv1, k1)
    m2 = mixer([alpha, gamma], 1)

    @pl.loop(0, rows // 2)
    def _(q):
        for u in range(2):
            r = q * 2 + u
            sol[r] = sol[r] + mix(m2, [R2, D1], r)
            res[r] = res[r] - mix(m2, [W2, S1], r)

    for p in range(3):
        for j in range(faces):
            halo(p, j).wait_send()

        @pl.loop(1, n)
        def _(k):
            gram_copy(p, lax.rem(me + k, n), me, k).wait_send()


def shards(right_side, band_blocks, link_blocks, link_rows):
    n = lax.axis_size("dom")
    rows, s, bs = right_side.shape
    faces, slots = link_blocks.shape[1:3]
    field = jax.ShapeDtypeStruct(right_side.shape, F32)
    any_spec = pl.BlockSpec(memory_space=pl.ANY)
    vmem = pl.BlockSpec(memory_space=pltpu.VMEM)
    return pl.pallas_call(
        functools.partial(kernel, n),
        out_shape=(field, field),
        in_specs=[pl.BlockSpec(memory_space=pltpu.SMEM), any_spec, any_spec, any_spec],
        out_specs=(vmem, vmem),
        scratch_shapes=[
            pltpu.VMEM((rows, s, bs), F32),
            pltpu.VMEM((rows, 5, bs, bs), F32),
            pltpu.VMEM((faces, slots, bs, bs), F32),
            pltpu.VMEM((rows + 4, 5 * bs, 2 * bs), BF16),
            pltpu.VMEM((faces * slots, bs, 2 * bs), BF16),
            pltpu.VMEM((NFIELD, rows + 4, 2 * s, bs), BF16),
            pltpu.VMEM((rows, s, bs), F32),
            pltpu.VMEM((rows, s, bs), F32),
            pltpu.VMEM((3, faces * slots, s, bs), F32),
            pltpu.VMEM((faces * slots + 1, s, bs), F32),
            pltpu.VMEM((faces * slots + 1, s, bs), F32),
            pltpu.VMEM((faces * slots + 1, s, bs), F32),
            pltpu.VMEM((3, s // 2, 128), F32),
            pltpu.VMEM((3, n, s // 2, 128), F32),
            pltpu.SMEM((rows * faces,), jnp.int32),
            pltpu.SemaphoreType.DMA((2 + rows // CHUNK,)),
            pltpu.SemaphoreType.DMA((3, faces)),
            pltpu.SemaphoreType.DMA((3, faces)),
            pltpu.SemaphoreType.DMA((3, n)),
            pltpu.SemaphoreType.DMA((3, n)),
        ],
        compiler_params=pltpu.CompilerParams(
            collective_id=0, has_side_effects=True, vmem_limit_bytes=60 * 1024 * 1024),
    )(link_rows, right_side, band_blocks, link_blocks)


def solution(mesh):
    in_specs = (
        P("dom", None, None),
        P("dom", None, None, None),
        P("dom", None, None, None, None),
        P("dom", None, None),
    )
    out_specs = (P("dom", None, None), P("dom", None, None))
    return jax.shard_map(shards, mesh=mesh, in_specs=in_specs, out_specs=out_specs, check_vma=False)
```

```python
import functools

import jax
import jax.numpy as jnp
from jax import lax
from jax.experimental import pallas as pl
from jax.experimental.pallas import tpu as pltpu
from jax.sharding import PartitionSpec as P

F32 = jnp.float32
BF16 = jnp.bfloat16
MESH = pl.DeviceIdType.MESH
CHUNK = 4
NFIELD = 10
R0, W0, Q0, R1, W1, Q1, D1, S1, R2, W2 = range(NFIELD)


def facing_offsets(dev_count):
    return (1, -1, dev_count // 16, -(dev_count // 16), dev_count // 4, -(dev_count // 4))


def split(x):
    hi = x.astype(BF16)
    lo = (x - hi.astype(F32)).astype(BF16)
    return hi, lo


def nn(a, b):
    return lax.dot_general(a, b, (((1,), (0,)), ((), ())), preferred_element_type=F32)


def nt(a, b):
    return lax.dot_general(a, b, (((1,), (1,)), ((), ())), preferred_element_type=F32)


def kernel(n, link_rows, rhs_hbm, band_hbm, link_hbm, sol, res,
           rhs, band, link, wt, lk, hl, wf, wband, hsend, hrecv0, hrecv1, hrecv2, gsend, gall, inv,
           load_sem, hs_sem, hr_sem, gs_sem, gr_sem):
    rows, s, bs = rhs.shape
    faces, slots = link.shape[:2]
    chunks = rows // CHUNK
    me = lax.axis_index("dom")
    offsets = facing_offsets(n)
    nslots = faces * slots
    hrecv = (hrecv0, hrecv1, hrecv2)

    rhs_copy = pltpu.make_async_copy(rhs_hbm, rhs, load_sem.at[0])
    link_copy = pltpu.make_async_copy(link_hbm.at[0], link, load_sem.at[1])

    def band_copy(c):
        at = pl.ds(c * CHUNK, CHUNK)
        return pltpu.make_async_copy(band_hbm.at[at], band.at[at], load_sem.at[2 + c])

    rhs_copy.start()
    link_copy.start()
    for c in range(chunks):
        band_copy(c).start()

    barrier = pltpu.get_barrier_semaphore()

    @pl.loop(1, n)
    def _(k):
        pl.semaphore_signal(barrier, inc=1, device_id=(lax.rem(me + k, n),), device_id_type=MESH)

    @pl.loop(0, rows)
    def _(r):
        for j in range(faces):
            found = jnp.int32(nslots)
            for t in range(slots):
                found = jnp.where(link_rows[0, t, j] == r, jnp.int32(j * slots + t), found)
            inv[r * faces + j] = found

    zero_pad = jnp.zeros((2 * s, bs), BF16)
    for f in (R0, W0, W1):
        for r in (0, 1, rows + 2, rows + 3):
            hl[f, r] = zero_pad
    zero_block = jnp.zeros((bs, 2 * bs), BF16)
    for r, m in ((2, 0), (2, 1), (3, 0), (rows, 4), (rows + 1, 3), (rows + 1, 4)):
        wt[r, m * bs:(m + 1) * bs, :] = zero_block
    for p in range(3):
        hrecv[p][nslots] = jnp.zeros((s, bs), F32)

    def put(f, r, x):
        hi, lo = split(x)
        hl[f, r + 2] = jnp.concatenate([hi, lo], axis=0)

    rhs_copy.wait()

    @pl.loop(0, rows // 4)
    def _(q):
        for u in range(4):
            r = q * 4 + u
            put(R0, r, rhs[r])

    link_copy.wait()

    @pl.loop(0, faces)
    def _(j):
        for t in range(slots):
            hi, lo = split(link[j, t])
            lk[j * slots + t] = jnp.concatenate([hi, lo], axis=1)

    def fold(x):
        half = x.shape[1] // 2
        y = x[:, :half] + x[:, half:]
        return y[:s] + y[s:]

    def halo(p, j):
        peer = lax.rem(me + offsets[j] + n, n)
        return pltpu.make_async_remote_copy(
            src_ref=hsend.at[p, pl.ds(j * slots, slots)],
            dst_ref=hrecv[p].at[pl.ds((j ^ 1) * slots, slots)],
            send_sem=hs_sem.at[p, j], recv_sem=hr_sem.at[p, j ^ 1],
            device_id=(peer,), device_id_type=MESH)

    def halo_arrived(p, j):
        return pltpu.make_async_remote_copy(
            src_ref=hsend.at[p, pl.ds(j * slots, slots)],
            dst_ref=hrecv[p].at[pl.ds(j * slots, slots)],
            send_sem=hs_sem.at[p, j], recv_sem=hr_sem.at[p, j],
            device_id=(me,), device_id_type=MESH)

    def halo_products(p, f):
        for j in range(faces):
            for t in range(slots):
                v = hl[f, link_rows[0, t, j] + 2]
                hsend[p, j * slots + t] = fold(nn(v, lk[j * slots + t]))

    def halo_start(p):
        for j in (4, 5, 2, 3, 0, 1):
            halo(p, j).start()

    def band_rows(f, first):
        none = jnp.zeros((2 * s, bs), BF16)
        deep = 4 * bs
        for u in range(0, CHUNK, 2):
            r = first + u
            v = [hl[f, r + m] for m in range(6)]
            pair = jnp.concatenate([jnp.concatenate([v[4], none], axis=1),
                                    jnp.concatenate([none, v[5]], axis=1)], axis=0)
            last = nn(pair, jnp.concatenate([wt[r + 2, deep:], wt[r + 3, deep:]], axis=0))
            for i in range(2):
                y = nn(jnp.concatenate(v[i:i + 4], axis=1), wt[r + 2 + i, :deep])
                wband[r + i] = fold(y + last[2 * s * i:2 * s * (i + 1)])

    def collect(p, f, keep):
        for j in range(faces):
            halo_arrived(p, j).wait_recv()

        @pl.loop(0, rows // 4)
        def _(q):
            for u in range(4):
                r = q * 4 + u
                w = wband[r]
                for j in range(faces):
                    w = w + hrecv[p][inv[r * faces + j]]
                if keep:
                    wf[r] = w
                put(f, r, w)

    lane = lax.broadcasted_iota(jnp.int32, (s, 128), 1)
    lane8 = lax.broadcasted_iota(jnp.int32, (s // 2, 128), 1)
    sub = lax.broadcasted_iota(jnp.int32, (s, 128), 0)

    def only(x):
        return jnp.where(lane < s, x, 0.0)

    def roll(x, by):
        return pltpu.roll(x, by % 128, 1)

    def gram_start(p, fr, fw, fd):
        def body(q, acc):
            for u in range(2):
                a = 4 * q + 2 * u + 2
                right = jnp.concatenate(
                    [jnp.concatenate([hl[f, a], hl[f, a + 1]], axis=1) for f in (fr, fw, fd)]
                    + [jnp.zeros((2 * s, 2 * bs), BF16)], axis=0)
                acc = acc + nt(right[:4 * s], right)
            return acc
        c = lax.fori_loop(0, rows // 4, body, jnp.zeros((4 * s, 128), F32))
        cr = c[:s] + c[s:2 * s]
        cw = c[2 * s:3 * s] + c[3 * s:]
        tr = cr + roll(cr, -s)
        tw = cw + roll(cw, -s)
        g = jnp.where(lane < s, tr, jnp.where(lane < 2 * s, roll(tw, -3 * s), jnp.where(lane < 3 * s, tr, 0.0)))
        msg = g[:s // 2] + roll(g[s // 2:], 64)
        gsend[p] = msg
        gall[p, me] = msg

        @pl.loop(1, n)
        def _(k):
            gram_copy(p, lax.rem(me + k, n), me, k).start()

    def gram_copy(p, peer, source, k):
        return pltpu.make_async_remote_copy(
            src_ref=gsend.at[p], dst_ref=gall.at[p, source],
            send_sem=gs_sem.at[p, k], recv_sem=gr_sem.at[p, source],
            device_id=(peer,), device_id_type=MESH)

    def gram_sum(p):
        @pl.loop(1, n)
        def _(k):
            source = lax.rem(me + k, n)
            gram_copy(p, source, source, k).wait_recv()
        total = jnp.sum(gall[p], axis=0)
        full = jnp.concatenate([jnp.where(lane8 < 64, total, 0.0),
                                jnp.where(lane8 < 64, roll(total, 64), 0.0)], axis=0)
        return only(full), only(roll(full, -s)), only(roll(full, -2 * s))

    def transpose(x):
        tall = jnp.concatenate([x, jnp.zeros((128 - s, 128), F32)], axis=0)
        return jnp.transpose(tall)[:s]

    def sym(x):
        return 0.5 * (x + transpose(x))

    def mul(a, b):
        return lax.dot_general(a[:, :s], b, (((1,), (0,)), ((), ())),
                               precision=lax.Precision.HIGHEST, preferred_element_type=F32)

    def solve(g, c):
        m = g + roll(c, s)
        for k in range(s):
            row = m[k:k + 1, :]
            scaled = row / row[:, k:k + 1]
            m = jnp.where(sub == k, scaled, m - m[:, k:k + 1] * scaled)
        return only(roll(m, -s))

    def mixer(blocks, outs):
        tall = [b for b in blocks for _ in range(2)]
        depth = s * len(tall)
        tall = tall + [jnp.zeros((128 - depth, 128), F32)]
        t = jnp.transpose(jnp.concatenate(tall, axis=0))[:outs * s]
        t = jnp.concatenate([roll(t, depth * g) if g else t for g in range(128 // depth)], axis=0)
        hi, lo = split(t)
        return jnp.concatenate([hi, lo], axis=0)

    def mix(m, fields, r):
        group = 128 // (2 * s * len(fields))
        u = jnp.concatenate([
            jnp.concatenate([hl[f, r + side * group + g + 2] for g in range(group) for f in fields], axis=0)
            for side in range(2)], axis=1)
        y = nn(m, u)
        half = y.shape[0] // 2
        y = y[:half] + y[half:]
        tall = half // group
        return [y[g * tall:(g + 1) * tall, side * bs:(side + 1) * bs]
                for side in range(2) for g in range(group)]

    halo_products(0, R0)
    pl.semaphore_wait(barrier, n - 1)
    halo_start(0)

    def convert(c):
        band_copy(c).wait()

        @pl.loop(0, CHUNK)
        def _(u):
            h = c * CHUNK + u
            for b in range(5):
                hi, lo = split(band[h, b])
                wt[h + b, (4 - b) * bs:(5 - b) * bs, :bs] = hi
                wt[h + b, (4 - b) * bs:(5 - b) * bs, bs:] = lo

    convert(0)

    @pl.loop(1, chunks)
    def _(c):
        convert(c)
        band_rows(R0, (c - 1) * CHUNK)

    band_rows(R0, rows - CHUNK)
    collect(0, W0, True)

    def send_products(p, f):
        halo_products(p, f)
        halo_start(p)

    def apply(p, fin, fout):
        @pl.loop(0, rows // CHUNK)
        def _(q):
            band_rows(fin, q * CHUNK)
        collect(p, fout, False)

    send_products(1, W0)
    gram_start(0, R0, W0, R0)
    apply(1, W0, Q0)
    rr, _, rw = gram_sum(0)
    rr0 = sym(rr)
    k0 = sym(rw)
    alpha = solve(k0, rr0)
    m0 = mixer([alpha], 1)

    @pl.loop(0, rows // 8)
    def _(q):
        xs, rs, ws = [mix(m0, [f], q * 8) for f in (R0, W0, Q0)]
        for u in range(8):
            r = q * 8 + u
            sol[r] = xs[u]
            x = rhs[r] - rs[u]
            res[r] = x
            put(R1, r, x)
            w = wf[r] - ws[u]
            wf[r] = w
            put(W1, r, w)

    send_products(2, W1)
    gram_start(1, R1, W1, R0)
    eye = jnp.where(sub == lane, 1.0, 0.0).astype(F32)
    inv0 = solve(rr0, eye)
    apply(2, W1, Q1)

    def coefficients(p, inverse, curv):
        rr, wd, rw = gram_sum(p)
        fresh = sym(rr)
        beta = mul(inverse, fresh)
        beta_t = mul(fresh, inverse)
        curv = sym(rw + mul(2.0 * wd + mul(beta_t, curv), beta))
        alpha = solve(curv, fresh)
        return fresh, curv, beta, alpha, mul(beta, alpha)

    rr1, k1, beta, alpha, gamma = coefficients(1, inv0, k0)
    m1 = mixer([beta + roll(gamma, s), roll(alpha, s)], 2)

    @pl.loop(0, rows // 4)
    def _(q):
        ds, ss, zs = [mix(m1, f, q * 4) for f in ([R0, R1], [W0, W1], [Q0, Q1])]
        for u in range(4):
            r = q * 4 + u
            x = res[r]
            w = wf[r]
            put(D1, r, x + ds[u][:s])
            sol[r] = sol[r] + ds[u][s:]
            put(S1, r, w + ss[u][:s])
            x = x - ss[u][s:]
            res[r] = x
            put(R2, r, x)
            put(W2, r, w - zs[u][s:])

    gram_start(2, R2, W2, D1)
    inv1 = solve(rr1, eye)
    _, _, _, alpha, gamma = coefficients(2, inv1, k1)
    m2 = mixer([alpha, gamma], 1)

    @pl.loop(0, rows // 4)
    def _(q):
        xs, rs = [mix(m2, f, q * 4) for f in ([R2, D1], [W2, S1])]
        for u in range(4):
            r = q * 4 + u
            sol[r] = sol[r] + xs[u]
            res[r] = res[r] - rs[u]

    for p in range(3):
        for j in range(faces):
            halo(p, j).wait_send()

        @pl.loop(1, n)
        def _(k):
            gram_copy(p, lax.rem(me + k, n), me, k).wait_send()


def hand_over(a, b, c, d):
    c[...] = a[...]
    d[...] = b[...]


def shards(right_side, band_blocks, link_blocks, link_rows):
    n = lax.axis_size("dom")
    rows, s, bs = right_side.shape
    faces, slots = link_blocks.shape[1:3]
    field = jax.ShapeDtypeStruct(right_side.shape, F32)
    any_spec = pl.BlockSpec(memory_space=pl.ANY)
    vmem = pl.BlockSpec(memory_space=pltpu.VMEM)
    pair = pl.pallas_call(
        functools.partial(kernel, n),
        out_shape=(field, field),
        in_specs=[pl.BlockSpec(memory_space=pltpu.SMEM), any_spec, any_spec, any_spec],
        out_specs=(vmem, vmem),
        scratch_shapes=[
            pltpu.VMEM((rows, s, bs), F32),
            pltpu.VMEM((rows, 5, bs, bs), F32),
            pltpu.VMEM((faces, slots, bs, bs), F32),
            pltpu.VMEM((rows + 4, 5 * bs, 2 * bs), BF16),
            pltpu.VMEM((faces * slots, bs, 2 * bs), BF16),
            pltpu.VMEM((NFIELD, rows + 4, 2 * s, bs), BF16),
            pltpu.VMEM((rows, s, bs), F32),
            pltpu.VMEM((rows, s, bs), F32),
            pltpu.VMEM((3, faces * slots, s, bs), F32),
            pltpu.VMEM((faces * slots + 1, s, bs), F32),
            pltpu.VMEM((faces * slots + 1, s, bs), F32),
            pltpu.VMEM((faces * slots + 1, s, bs), F32),
            pltpu.VMEM((3, s // 2, 128), F32),
            pltpu.VMEM((3, n, s // 2, 128), F32),
            pltpu.SMEM((rows * faces,), jnp.int32),
            pltpu.SemaphoreType.DMA((2 + rows // CHUNK,)),
            pltpu.SemaphoreType.DMA((3, faces)),
            pltpu.SemaphoreType.DMA((3, faces)),
            pltpu.SemaphoreType.DMA((3, n)),
            pltpu.SemaphoreType.DMA((3, n)),
        ],
        compiler_params=pltpu.CompilerParams(
            collective_id=0, has_side_effects=True, vmem_limit_bytes=60 * 1024 * 1024),
    )(jnp.swapaxes(link_rows, 1, 2), right_side, band_blocks, link_blocks)

    return pl.pallas_call(
        hand_over, out_shape=(field, field), in_specs=[vmem, vmem], out_specs=(vmem, vmem))(*pair)


def solution(mesh):
    in_specs = (
        P("dom", None, None),
        P("dom", None, None, None),
        P("dom", None, None, None, None),
        P("dom", None, None),
    )
    out_specs = (P("dom", None, None), P("dom", None, None))
    return jax.shard_map(shards, mesh=mesh, in_specs=in_specs, out_specs=out_specs, check_vma=False)
```
